16 devices in a mesh: tp: 2 (over z), dp: 8 (over y, x, core).
Axes of the slice: x: 2, y: 2, z: 2, core: 2. Of those that a mesh axis runs over, the one named last changes fastest.
Arguments:
- hidden: bfloat16 [8192, 2048], P('dp')
- embedding: bfloat16 [49152, 2048], P('tp')
- norm_weight: float32 [2048], replicated
- teach_ids: int32 [8192, 256], P('dp')
- teach_prob: float32 [8192, 256], P('dp')
- tok_mask: float32 [8192], P('dp')
Outputs:
- output 1: float32 [], replicated
- output 2: bfloat16 [8192, 2048], P('dp')
- output 3: float32 [49152, 2048], P('tp', 'dp')
- output 4: float32 [2048], replicated
All inputs are finite; a program needn't handle non-finite values.
Results may differ from the reference program's by a relative error of at most 0.001.
Values sent between devices are 32-bit elements.
A program may use at most 1 GiB of HBM per device.

```python
import jax
import jax.numpy as jnp
from jax import lax

MODEL_DIM = 2048
VOCAB_SIZE = 49152
TEACH_TOP = 256
NUM_TOKENS = 8192

EPS_NORM = 1e-6
LOGIT_GAIN = 2.5
HALF_TOP = TEACH_TOP // 2
FREQ_VOCAB = VOCAB_SIZE // 8
ROW_BLOCK = min(NUM_TOKENS, 64)


def draw_teacher_ids(key_ids):
    key_low, key_high, key_perm = jax.random.split(key_ids, 3)
    low_band = FREQ_VOCAB // HALF_TOP
    high_band = (VOCAB_SIZE - FREQ_VOCAB) // HALF_TOP
    slot_pos = jnp.arange(HALF_TOP, dtype=jnp.int32)
    high_width = jnp.where(slot_pos == HALF_TOP - 1, VOCAB_SIZE - FREQ_VOCAB - (HALF_TOP - 1) * high_band, high_band)
    low_off = jax.random.randint(key_low, (NUM_TOKENS, HALF_TOP), 0, low_band, dtype=jnp.int32)
    high_raw = jax.random.randint(key_high, (NUM_TOKENS, HALF_TOP), 0, 1 << 24, dtype=jnp.int32)
    high_off = high_raw % high_width[None, :]
    low_off = low_off.at[0, 0].set(0)
    high_off = high_off.at[0, HALF_TOP - 1].set(high_width[HALF_TOP - 1] - 1)
    low_ids = slot_pos[None, :] * low_band + low_off
    high_ids = FREQ_VOCAB + slot_pos[None, :] * high_band + high_off
    all_ids = jnp.concatenate([low_ids, high_ids], axis=1)
    row_keys = jax.random.split(key_perm, NUM_TOKENS)
    perm_rows = jax.vmap(lambda row_key: jax.random.permutation(row_key, TEACH_TOP))(row_keys)
    return jnp.take_along_axis(all_ids, perm_rows.astype(jnp.int32), axis=1)


def draw_mask(key_mask):
    keep_flag = jax.random.randint(key_mask, (NUM_TOKENS,), 0, 8, dtype=jnp.int32) != 0
    return keep_flag.astype(jnp.float32).at[0].set(1.0)


def setup_inputs(seed: int = 0) -> dict:
    root_key = jax.random.key(seed)
    key_h, key_e, key_w, key_ids, key_prob, key_mask = jax.random.split(root_key, 6)
    hidden = jax.random.normal(key_h, (NUM_TOKENS, MODEL_DIM), jnp.float32).astype(jnp.bfloat16)
    embed_scale = LOGIT_GAIN * MODEL_DIM ** -0.5
    embedding = (jax.random.normal(key_e, (VOCAB_SIZE, MODEL_DIM), jnp.float32) * embed_scale).astype(jnp.bfloat16)
    norm_weight = 0.5 * jax.random.normal(key_w, (MODEL_DIM,), jnp.float32)
    teach_ids = draw_teacher_ids(key_ids)
    teach_prob = jax.nn.softmax(jax.random.normal(key_prob, (NUM_TOKENS, TEACH_TOP), jnp.float32), axis=1)
    tok_mask = draw_mask(key_mask)
    return {'hidden': hidden, 'embedding': embedding, 'norm_weight': norm_weight, 'teach_ids': teach_ids, 'teach_prob': teach_prob, 'tok_mask': tok_mask}


def reference(hidden, embedding, norm_weight, teach_ids, teach_prob, tok_mask):
    mask_total = jnp.sum(tok_mask)
    scale_w = 1.0 + norm_weight
    num_blocks = NUM_TOKENS // ROW_BLOCK
    row_ids = jnp.arange(ROW_BLOCK)[:, None]

    def block_step(acc_embed, block_in):
        h_blk, ids_blk, prob_blk, mask_blk = block_in
        h_f32 = h_blk.astype(jnp.float32)
        inv_rms = lax.rsqrt(jnp.mean(h_f32 * h_f32, axis=1, keepdims=True) + EPS_NORM)
        normed = h_f32 * inv_rms
        normed_bf = (normed * scale_w).astype(jnp.bfloat16)
        logits = lax.dot_general(normed_bf, embedding, (((1,), (1,)), ((), ())), preferred_element_type=jnp.float32)
        row_max = jnp.max(logits, axis=1, keepdims=True)
        log_norm = row_max + jnp.log(jnp.sum(jnp.exp(logits - row_max), axis=1, keepdims=True))
        picked = jnp.take_along_axis(logits, ids_blk, axis=1)
        teach_sum = jnp.sum(prob_blk * picked, axis=1)
        loss_part = jnp.sum(mask_blk * (teach_sum - log_norm[:, 0]))
        weight = (mask_blk / mask_total)[:, None]
        soft_prob = jnp.exp(logits - log_norm)
        d_logits = (soft_prob * weight).at[row_ids, ids_blk].add(-prob_blk * weight)
        dlogit_bf = d_logits.astype(jnp.bfloat16)
        grad_u = jnp.dot(dlogit_bf, embedding, preferred_element_type=jnp.float32)
        acc_embed = acc_embed + lax.dot_general(dlogit_bf, normed_bf, (((0,), (0,)), ((), ())), preferred_element_type=jnp.float32)
        d_normed = grad_u * scale_w
        grad_h = inv_rms * (d_normed - normed * jnp.mean(d_normed * normed, axis=1, keepdims=True))
        grad_w = jnp.sum(grad_u * normed, axis=0)
        return acc_embed, (loss_part, grad_h.astype(jnp.bfloat16), grad_w)

    blocks = (hidden.reshape(num_blocks, ROW_BLOCK, MODEL_DIM), teach_ids.reshape(num_blocks, ROW_BLOCK, TEACH_TOP), teach_prob.reshape(num_blocks, ROW_BLOCK, TEACH_TOP), tok_mask.reshape(num_blocks, ROW_BLOCK))
    acc_init = jnp.zeros((VOCAB_SIZE, MODEL_DIM), jnp.float32)
    grad_embed, (loss_parts, grad_hidden, norm_parts) = lax.scan(block_step, acc_init, blocks)
    loss_mean = -jnp.sum(loss_parts) / mask_total
    return loss_mean, grad_hidden.reshape(NUM_TOKENS, MODEL_DIM), grad_embed, jnp.sum(norm_parts, axis=0)
```

```python
import functools

import jax
import jax.numpy as jnp
from jax import lax
from jax.experimental import pallas as pl
from jax.experimental.pallas import tpu as pltpu
from jax.sharding import PartitionSpec as P

EPS_NORM = 1e-6
LANES = 128
NT = (((1,), (1,)), ((), ()))
TN = (((0,), (0,)), ((), ()))
ORDER = (7, 5, 3, 1, 6, 4, 2, 0)


def flip(value, bit):
    return lax.ppermute(value, 'dp', [(i, i ^ bit) for i in range(8)])


def logits_body(start_ref, u_ref, e_ref, z_ref, m_ref, l_ref):
    rows, width = z_ref.shape

    @pl.when(pl.program_id(0) == 0)
    def _():
        m_ref[...] = jnp.full(m_ref.shape, -jnp.inf, jnp.float32)
        l_ref[...] = jnp.zeros(l_ref.shape, jnp.float32)

    z_ref[...] = lax.dot_general(u_ref[...], e_ref[...], NT, preferred_element_type=jnp.float32)

    def step(i, carry):
        at = pl.ds(pl.multiple_of(i * 32, 32), 32)
        parts = [z_ref[at, c * LANES:(c + 1) * LANES] for c in range(width // LANES)]
        old = m_ref[at, :]
        top = functools.reduce(jnp.maximum, parts, old)
        total = l_ref[at, :] * jnp.exp(old - top)
        for part in parts:
            total = total + jnp.exp(part - top)
        m_ref[at, :] = top
        l_ref[at, :] = total
        return carry

    lax.fori_loop(0, rows // 32, step, 0)


def logits_alias_body(start_ref, u_ref, e_ref, old_ref, z_ref, m_ref, l_ref):
    logits_body(start_ref, u_ref, e_ref, z_ref, m_ref, l_ref)


def logits_call(start, u, e, half, z_old, width, tile):
    rows, depth = u.shape
    in_specs = [
        pl.BlockSpec((rows, depth), lambda j, s: (0, 0)),
        pl.BlockSpec((tile, depth), lambda j, s: (s[0] + j, 0)),
    ]
    operands = [start, u, e]
    aliases = {}
    if z_old is not None:
        in_specs.append(pl.BlockSpec(memory_space=pl.ANY))
        operands.append(z_old)
        aliases = {3: 0}
    stat = pl.BlockSpec((rows, LANES), lambda j, s: (0, 0))
    return pl.pallas_call(
        logits_body if z_old is None else logits_alias_body,
        grid_spec=pltpu.PrefetchScalarGridSpec(
            num_scalar_prefetch=1,
            grid=(width // tile,),
            in_specs=in_specs,
            out_specs=[pl.BlockSpec((rows, tile), lambda j, s: (half, j)), stat, stat],
        ),
        out_shape=[
            jax.ShapeDtypeStruct((2 * rows, width), jnp.float32),
            jax.ShapeDtypeStruct((rows, LANES), jnp.float32),
            jax.ShapeDtypeStruct((rows, LANES), jnp.float32),
        ],
        input_output_aliases=aliases,
        compiler_params=pltpu.CompilerParams(dimension_semantics=('arbitrary',), vmem_limit_bytes=50 * 2 ** 20),
        cost_estimate=pl.CostEstimate(flops=2 * rows * width * depth, bytes_accessed=width * depth * 2 + rows * width * 4, transcendentals=rows * width),
    )(*operands)


PLAN = (
    'g0', 'c0', 'g1', 'y0', 'c1', 'o0', 'y1', 'g2', 'c2', 'o1', 'y2', 's0', 'c3', 'o2', 'y3',
    'g3', 's1', 'p0', 'p1', 'c4', 'o3', 'y4', 'd0', 's2', 'c5', 'o4', 'y5', 'd1', 's3', 'c6',
    'o5', 'y6', 'c7', 'o6', 'y7', 'o7', 's4', 's5', 's6', 's7',
)


GROUP = 16
PITCH = 104


def teach_body(hi_ref, lo_ref, pt_ref, out_ref, scr_ref):
    tokens, width = out_ref.shape
    count = width // LANES
    top = hi_ref.shape[1]
    hi_iota = lax.broadcasted_iota(jnp.int32, (count, top), 0)
    lo_iota = lax.broadcasted_iota(jnp.int32, (LANES, top), 0)

    def step(i, carry):
        for sub in range(GROUP // 8):
            row = pl.multiple_of(i * GROUP + sub * 8, 8)
            hi8 = hi_ref[pl.ds(row, 8), :]
            lo8 = lo_ref[pl.ds(row, 8), :]
            rest = pt_ref[pl.ds(row, 8), :]
            one = rest.astype(jnp.bfloat16).astype(jnp.float32)
            rest = rest - one
            two = rest.astype(jnp.bfloat16).astype(jnp.float32)
            three = rest - two
            for t in range(8):
                hit = hi8[t:t + 1, :] == hi_iota
                left = jnp.concatenate([jnp.where(hit, piece[t:t + 1, :], 0.0).astype(jnp.bfloat16) for piece in (one, two, three)], axis=0)
                right = jnp.where(lo8[t:t + 1, :] == lo_iota, 1.0, 0.0).astype(jnp.bfloat16)
                dense = lax.dot_general(left, right, NT, preferred_element_type=jnp.float32)
                scr_ref[pl.ds((sub * 8 + t) * PITCH, count), :] = dense[:count] + dense[count:2 * count] + dense[2 * count:]
        for sub in range(GROUP // 8):
            row = pl.multiple_of(i * GROUP + sub * 8, 8)
            for h in range(count):
                out_ref[pl.ds(row, 8), h * LANES:(h + 1) * LANES] = scr_ref[pl.ds(sub * 8 * PITCH + h, 8, stride=PITCH), :]
        return carry

    lax.fori_loop(0, tokens // GROUP, step, 0)


def teach_alias_body(hi_ref, lo_ref, pt_ref, old_ref, out_ref, scr_ref):
    teach_body(hi_ref, lo_ref, pt_ref, out_ref, scr_ref)


def teach_call(hi, lo, pt, half, old, width, block):
    rows, top = hi.shape
    steps = rows // block
    spec = pl.BlockSpec((block, top), lambda i: (i, 0))
    in_specs, operands, aliases = [spec] * 3, [hi, lo, pt], {}
    if old is not None:
        in_specs.append(pl.BlockSpec(memory_space=pl.ANY))
        operands.append(old)
        aliases = {3: 0}
    return pl.pallas_call(
        teach_body if old is None else teach_alias_body,
        grid=(steps,),
        in_specs=in_specs,
        out_specs=pl.BlockSpec((block, width), lambda i: (half * steps + i, 0)),
        out_shape=jax.ShapeDtypeStruct((2 * rows, width), jnp.float32),
        scratch_shapes=[pltpu.VMEM((GROUP * PITCH, LANES), jnp.float32)],
        input_output_aliases=aliases,
        compiler_params=pltpu.CompilerParams(dimension_semantics=('arbitrary',), vmem_limit_bytes=40 * 2 ** 20),
        cost_estimate=pl.CostEstimate(flops=6 * rows * width * top, bytes_accessed=rows * width * 4, transcendentals=0),
    )(*operands)


def grad_body(z_ref, p_ref, lz_ref, w_ref, g_ref, t_ref):
    rows, width = z_ref.shape

    @pl.when((pl.program_id(0) == 0) & (pl.program_id(1) == 0))
    def _():
        t_ref[...] = jnp.zeros(t_ref.shape, jnp.float32)

    def step(i, acc):
        at = pl.ds(pl.multiple_of(i * 32, 32), 32)
        lz = lz_ref[at, :]
        w = w_ref[at, :]
        for c in range(width // LANES):
            cols = slice(c * LANES, (c + 1) * LANES)
            z = z_ref[at, cols]
            wp = p_ref[at, cols] * w
            g_ref[at, cols] = (jnp.exp(z - lz) * w - wp).astype(jnp.bfloat16)
            acc = acc + wp * z
        return acc

    acc = lax.fori_loop(0, rows // 32, step, jnp.zeros((32, LANES), jnp.float32))
    t_ref[...] += acc


def grad_call(z, p, log_norm, weight, first, width, rows, tile):
    total = z.shape[0]
    base = first // tile
    wide = pl.BlockSpec((rows, tile), lambda i, j: (i, base + j))
    stat = pl.BlockSpec((rows, LANES), lambda i, j: (i, 0))
    return pl.pallas_call(
        grad_body,
        grid=(total // rows, width // tile),
        in_specs=[wide, wide, stat, stat],
        out_specs=[pl.BlockSpec((rows, tile), lambda i, j: (i, j)), pl.BlockSpec((32, LANES), lambda i, j: (0, 0))],
        out_shape=[jax.ShapeDtypeStruct((total, width), jnp.bfloat16), jax.ShapeDtypeStruct((32, LANES), jnp.float32)],
        compiler_params=pltpu.CompilerParams(dimension_semantics=('arbitrary', 'arbitrary'), vmem_limit_bytes=40 * 2 ** 20),
        cost_estimate=pl.CostEstimate(flops=100 * total * width, bytes_accessed=total * width * 10, transcendentals=total * width),
    )(z, p, log_norm, weight)


def solution(mesh):
    def local_head(hidden, embedding, norm_weight, teach_ids, teach_prob, tok_mask):
        quarter = embedding.shape[0] // 2
        tok, depth = hidden.shape
        block = depth // 8
        dp, tp = lax.axis_index('dp'), lax.axis_index('tp')
        side = (dp >> 1) & 1
        base = tp * embedding.shape[0] + side * quarter

        scale_w = 1.0 + norm_weight
        h_f32 = hidden.astype(jnp.float32)
        inv_rms = lax.rsqrt(jnp.mean(h_f32 * h_f32, axis=1, keepdims=True) + EPS_NORM)
        normed = h_f32 * inv_rms
        mask_total = lax.psum(jnp.sum(tok_mask), 'dp')
        half = tok // 2

        def swap_z(value):
            return lax.ppermute(value, 'tp', [(0, 1), (1, 0)])

        def both_halves(near, far):
            first, second = jnp.where(tp == 0, near, far), jnp.where(tp == 0, far, near)
            return jnp.concatenate([first, second], axis=0)

        mask_pair = flip(tok_mask, 2)
        x_ids = flip(lax.dynamic_slice_in_dim(teach_ids, tp * half, half), 2)
        x_prob = flip(lax.dynamic_slice_in_dim(teach_prob, tp * half, half), 2)
        x_act = [flip(lax.dynamic_slice_in_dim(normed, tp * half + c * (half // 2), half // 2), 2) for c in range(2)]
        z_ids, z_prob = swap_z(x_ids), swap_z(x_prob)
        z_act = [swap_z(x_act[c]) for c in range(2)]
        normed_pair = both_halves(jnp.concatenate(x_act, axis=0), jnp.concatenate(z_act, axis=0))
        u_own = (normed * scale_w).astype(jnp.bfloat16)
        u_pair = (normed_pair * scale_w).astype(jnp.bfloat16)

        def split_ids(ids):
            near = ids - base
            ok = (near >= 0) & (near < quarter)
            return jnp.where(ok, near >> 7, -1), near & (LANES - 1)

        tile = 1024
        start = (side * (quarter // tile)).reshape(1).astype(jnp.int32)
        z, max_own, sum_own = logits_call(start, u_own, embedding, 0, None, quarter, tile)
        first_ids, _ = lax.optimization_barrier((teach_ids, max_own))
        dense = teach_call(*split_ids(first_ids), teach_prob, 0, None, quarter, min(64, tok))
        x_ids, x_prob, z_ids, z_prob, dense = lax.optimization_barrier((x_ids, x_prob, z_ids, z_prob, dense))
        ids_pair, prob_pair = both_halves(x_ids, z_ids), both_halves(x_prob, z_prob)
        dense = teach_call(*split_ids(ids_pair), prob_pair, 1, dense, quarter, min(64, tok))
        u_pair, dense, z = lax.optimization_barrier((u_pair, dense, z))
        z, max_pair, sum_pair = logits_call(start, u_pair, embedding, 1, z, quarter, tile)

        def lane_merge(top, total):
            best = jnp.max(top, axis=1)
            return best, jnp.sum(total * jnp.exp(top - best[:, None]), axis=1)

        own, pair = jnp.stack(lane_merge(max_own, sum_own)), jnp.stack(lane_merge(max_pair, sum_pair))
        stats = jnp.concatenate([own, pair], axis=1)
        swapped = jnp.concatenate([pair, own], axis=1)
        both = [(i, (i ^ 2) ^ 8) for i in range(16)]
        shards = [stats, flip(swapped, 2), lax.ppermute(stats, 'tp', [(0, 1), (1, 0)]), lax.ppermute(swapped, ('tp', 'dp'), both)]
        best = functools.reduce(jnp.maximum, [s[0] for s in shards])
        log_norm = best + jnp.log(sum(s[1] * jnp.exp(s[0] - best) for s in shards))
        weight = jnp.concatenate([tok_mask, mask_pair]) / mask_total
        lz_wide = jnp.broadcast_to(log_norm[:, None], (2 * tok, LANES))
        w_wide = jnp.broadcast_to(weight[:, None], (2 * tok, LANES))

        size = quarter // 8
        u_all = jnp.concatenate([u_own, u_pair], axis=0)
        u_parts = [
            jnp.concatenate([lax.dynamic_slice(u_all, (0, (dp ^ r) * block), (2 * tok, block)) for r in group], axis=1)
            for group in (ORDER[:4], ORDER[4:6], ORDER[6:])
        ]

        last = [log_norm]

        def after(value):
            return lax.optimization_barrier((value, last[0]))[0]

        def mark(value):
            last[0] = value
            return value

        pieces = ((0, 1), (1, 1), (2, 2), (4, 4))
        grads, scores = {}, []
        core, half_y, half_o = {}, {}, {}

        def grad_step(k):
            first, count = pieces[k]
            g, score = grad_call(z, dense, after(lz_wide), w_wide, first * size, count * size, min(512, 2 * tok), 1536)
            mark(score)
            scores.append(score)
            for j in range(first, first + count):
                grads[j] = g[:, (j - first) * size:(j - first + 1) * size]
            grads['piece', k] = g

        def embed_dot(j, k):
            return lax.dot_general(grads[j], after(u_parts[k]), TN, preferred_element_type=jnp.float32)

        def core_step(j):
            core[j] = flip(mark(embed_dot(j, 0)), 1)

        def y_step(j):
            half_y[j] = flip(mark(embed_dot(j, 1) + core[j][:, :2 * block]), 4)

        def own_step(j):
            half_o[j] = mark(embed_dot(j, 2) + core[j][:, 2 * block:])

        x_rows = {}
        grad_embed = [jnp.zeros((2 * quarter, block), jnp.float32)]

        def place(rows, row):
            grad_embed[0] = lax.dynamic_update_slice(grad_embed[0], rows, (row, 0))

        def place_x(j):
            rows, grad_embed[0] = lax.optimization_barrier((x_rows[j], grad_embed[0]))
            place(rows, (1 - side) * quarter + j * size)

        def sum_step(j):
            own, from_y = lax.optimization_barrier((after(half_o[j]), half_y[j]))
            x_rows[j] = flip(own[:, :block] + from_y[:, :block], 2)
            place(mark(own[:, block:] + from_y[:, block:]), side * quarter + j * size)
            if j >= 3:
                place_x(j - 3)

        half_depth = depth // 2
        from_x, grad_half = {}, {}

        def du_dot(row, col):
            total = None
            for k, (first, count) in enumerate(pieces):
                e = lax.dynamic_slice(embedding, (side * quarter + first * size, col), (count * size, half_depth))
                g = grads['piece', k][row:row + tok]
                term = jnp.dot(after(g) if k == 0 else g, e, preferred_element_type=jnp.float32)
                total = term if total is None else total + term
            return total

        def pair_step(i):
            from_x[i] = flip(mark(du_dot(tok, i * half_depth)), 2)

        def du_step(i):
            total = mark(du_dot(0, i * half_depth) + from_x[i])
            other = lax.ppermute(total, 'tp', [(0, 1), (1, 0)])
            grad_half[i] = total + other

        steps = {'g': grad_step, 'c': core_step, 'y': y_step, 'o': own_step, 's': sum_step, 'p': pair_step, 'd': du_step}
        for word in PLAN:
            steps[word[0]](int(word[1:]))
        for j in range(5, 8):
            place_x(j)
        grad_embed = grad_embed[0]

        grad_u = jnp.concatenate([grad_half[0], grad_half[1]], axis=1)
        d_normed = grad_u * scale_w
        grad_hidden = (inv_rms * (d_normed - normed * jnp.mean(d_normed * normed, axis=1, keepdims=True))).astype(jnp.bfloat16)
        grad_norm = lax.psum(jnp.sum(grad_u * normed, axis=0), 'dp')
        score = sum(jnp.sum(part) for part in scores) - 0.5 * jnp.sum(weight[:tok] * log_norm[:tok])
        loss_mean = -lax.psum(score, ('tp', 'dp'))
        return loss_mean, grad_hidden, grad_embed, grad_norm

    return jax.shard_map(local_head, mesh=mesh, in_specs=(P('dp', None), P('tp', None), P(None), P('dp', None), P('dp', None), P('dp')), out_specs=(P(), P('dp', None), P('tp', 'dp'), P(None)), check_vma=False)
```
